32 devices in a mesh: zero: 8 (over y, x, core), cols: 4 (over z).
Axes of the slice: x: 2, y: 2, z: 4, core: 2. Of those that a mesh axis runs over, the one named last changes fastest.
Arguments:
- train_gate: bfloat16 [4096, 11008], P('zero', 'cols'), may hold values from -0.125 to 0.125
- low_gate: bfloat16 [4096, 64], P('zero'), may hold values from -0.09375 to 0.09375
- high_gate: bfloat16 [64, 11008], P(None, 'cols'), may hold values from -0.75 to 0.75
- train_up: bfloat16 [4096, 11008], P('zero', 'cols'), may hold values from -0.125 to 0.125
- low_up: bfloat16 [4096, 64], P('zero'), may hold values from -0.09375 to 0.09375
- high_up: bfloat16 [64, 11008], P(None, 'cols'), may hold values from -0.75 to 0.75
- norm_train: float32 [4096], P(('zero', 'cols')), may hold values from 0.25 to 1.75
- norm_step: float32 [4096], P(('zero', 'cols')), may hold values from -0.3 to 0.3
Outputs:
- ready_gate: bfloat16 [4096, 11008], P(None, 'cols')
- ready_up: bfloat16 [4096, 11008], P(None, 'cols')
- factor_gate: float32 [11008], P('cols')
- factor_up: float32 [11008], P('cols')
- serve_norm: bfloat16 [4096], replicated
The draws below stay inside these ranges and needn't reach their ends.
All inputs are finite; a program needn't handle non-finite values. Where the reference program divides by a largest or mean magnitude, that divisor is 1e-20 or more.
Results may differ from the reference program's by a relative error of at most 0.001.
Values may be sent and summed in bfloat16 or wider, within the bound.
A program may use at most 192 MiB of HBM per device.

```python
import jax
import jax.numpy as jnp

D_MODEL = 4096
D_INNER = 11008
RANK = 64


def strengthened(values, stream_key, source, target, parts, factor):
    def block_of(axis_at):
        return (jnp.arange(values.shape[axis_at]) // (values.shape[axis_at] // parts)).reshape((-1,) + (1,) * (values.ndim - 1 - axis_at))

    near = jax.random.permutation(stream_key, parts)[block_of(target)]
    far = (block_of(target) + parts // 2) % parts
    return jnp.where((block_of(source) == near) | (block_of(source) == far), factor * values, values)


def steps_of(key, dims, cuts, smallest, top_value):
    gain = 1.0
    for axis_at, parts in cuts:
        steps = jax.random.uniform(jax.random.fold_in(jax.random.fold_in(key, 6), axis_at), (parts,), jnp.float32, smallest / len(cuts), top_value / len(cuts))
        gain = gain * jnp.repeat(jnp.exp(steps), dims[axis_at] // parts).reshape((-1,) + (1,) * (len(dims) - 1 - axis_at))
    return gain


def noise(stream_key, dims, scale, bound, cuts=(), kind=jnp.bfloat16):
    entries = scale * jax.random.normal(stream_key, dims, jnp.float32)
    if cuts:
        entries = entries * steps_of(stream_key, dims, cuts, -0.22, 0.18)
    return jnp.clip(entries, -bound, bound).astype(kind)


def bell_draw_with(own_key, shape, width, reach, pieces, heavy, kind=jnp.bfloat16):
    result = width * jax.random.normal(own_key, shape, jnp.float32)
    if pieces:
        result = result * steps_of(own_key, shape, pieces, -0.22, 0.18)
    return jnp.clip(strengthened(result, jax.random.fold_in(own_key, 3), *heavy), -reach, reach).astype(kind)


def setup_inputs(seed: int = 0) -> dict:
    arg_keys = jax.random.split(jax.random.key(seed), 9)
    return {
        "train_gate": bell_draw_with(arg_keys[0], (D_MODEL, D_INNER), D_MODEL ** -0.5, 0.125, ((0, 8), (1, 4)), (0, 1, 8, 2.0)),
        "low_gate": noise(arg_keys[1], (D_MODEL, RANK), D_MODEL ** -0.5, 0.09375, ((0, 8),)),
        "high_gate": noise(arg_keys[2], (RANK, D_INNER), RANK ** -0.5, 0.75, ((1, 4),)),
        "train_up": bell_draw_with(arg_keys[3], (D_MODEL, D_INNER), D_MODEL ** -0.5, 0.125, ((0, 8), (1, 4)), (0, 1, 8, 2.0)),
        "low_up": noise(arg_keys[4], (D_MODEL, RANK), D_MODEL ** -0.5, 0.09375, ((0, 8),)),
        "high_up": noise(arg_keys[5], (RANK, D_INNER), RANK ** -0.5, 0.75, ((1, 4),)),
        "norm_train": jnp.clip(1.0 + 0.15 * jax.random.normal(arg_keys[6], (D_MODEL,), jnp.float32), 0.25, 1.75),
        "norm_step": jnp.clip(jax.random.uniform(arg_keys[7], (D_MODEL,), jnp.float32, -0.3, 0.3) * steps_of(arg_keys[7], (D_MODEL,), ((0, 32),), -0.4, 0.0), -0.3, 0.3),
    }


mix_rate = 1.0


def reference(train_gate, low_gate, high_gate, train_up, low_up, high_up, norm_train, norm_step):
    latest_gate = train_gate.astype(jnp.float32) + mix_rate * jnp.dot(low_gate, high_gate, preferred_element_type=jnp.float32)
    latest_up = train_up.astype(jnp.float32) + mix_rate * jnp.dot(low_up, high_up, preferred_element_type=jnp.float32)
    factor_gate = jnp.sum(jnp.abs(latest_gate), axis=0) / D_MODEL
    ready_gate = (latest_gate / factor_gate).astype(jnp.bfloat16)
    factor_up = jnp.sum(jnp.abs(latest_up), axis=0) / D_MODEL
    ready_up = (latest_up / factor_up).astype(jnp.bfloat16)
    serve_norm = (norm_train + norm_step).astype(jnp.bfloat16)
    return ready_gate, ready_up, factor_gate, factor_up, serve_norm
```

```python
import functools

import jax
import jax.numpy as jnp
from jax import lax
from jax.experimental import pallas as pl
from jax.experimental.pallas import tpu as pltpu
from jax.sharding import PartitionSpec as P

mix_rate = 1.0
CHUNKS = 4
WINDOW = 4
LANES = 128
TILE = 16
BLOCK = 704
MESH = pl.DeviceIdType.MESH

OWN_X, OWN_Y, OWN_S, DIAG, X_S, Y_S, D_S = range(7)


def one_half(low, i):
    rank = low.shape[0] // 2
    mine, none = low[i * rank:(i + 1) * rank], jnp.zeros((rank, low.shape[1]), low.dtype)
    return jnp.concatenate([none, mine] if i else [mine, none], axis=0)


def gather_kernel(
    n, cols, axes,
    gate, up, low, high, norm,
    all_gate, all_up, all_low, total, scale, all_norm,
    own_gate, own_up, own_low, vhigh, part, landed,
    send, recv, local_sem, sum_send, sum_recv, norm_send, norm_recv, z_send, z_recv,
):
    zero_axis, cols_axis = axes
    me, col = lax.axis_index(zero_axis), lax.axis_index(cols_axis)
    core, x, y = me % 2, (me // 2) % 2, me // 4
    to_s, to_x, to_y = 1 - 2 * core, 2 - 4 * x, 4 - 8 * y
    sib, xn, yn = me + to_s, me + to_x, me + to_y
    diag = xn + to_y
    width = gate.shape[0]
    d_model = n * gate.shape[1]

    barrier = pltpu.get_barrier_semaphore()
    for peer in (sib, xn, yn):
        pl.semaphore_signal(barrier, inc=1, device_id={zero_axis: peer, cols_axis: col}, device_id_type=MESH)
    for step in range(1, cols):
        pl.semaphore_signal(
            barrier, inc=1, device_id={zero_axis: me, cols_axis: (col + step) % cols}, device_id_type=MESH
        )
    pl.semaphore_wait(barrier, 3 + cols - 1)

    size = width // CHUNKS
    half = low.shape[0] // 2
    pieces = [(low, all_low, 0, half), (low, all_low, half, half)]
    for k in range(CHUNKS):
        pieces += [(gate, all_gate, k * size, size), (up, all_up, k * size, size)]
    count = len(pieces)

    def place(p, owner):
        _, out, start, length = pieces[p]
        return out.at[owner, pl.ds(start, length)]

    def own(p):
        ref, _, start, length = pieces[p]
        return ref.at[pl.ds(start, length)]

    def copy(kind, p, src, owner, target):
        return pltpu.make_async_remote_copy(
            src_ref=src,
            dst_ref=place(p, owner),
            send_sem=send.at[kind, p],
            recv_sem=recv.at[kind, p],
            device_id={zero_axis: target, cols_axis: col},
            device_id_type=MESH,
        )

    started = []

    def go(c):
        c.start()
        started.append(c)

    def send_own(p):
        go(copy(OWN_X, p, own(p), me, xn))
        go(copy(OWN_Y, p, own(p), me, yn))
        go(copy(OWN_S, p, own(p), me, sib))

    for p in range(WINDOW):
        send_own(p)

    def z_copy(step):
        return pltpu.make_async_remote_copy(
            src_ref=norm,
            dst_ref=all_norm.at[me, col],
            send_sem=z_send.at[step],
            recv_sem=z_recv.at[step],
            device_id={zero_axis: me, cols_axis: (col + step) % cols},
            device_id_type=MESH,
        )

    for step in range(1, cols):
        go(z_copy(step))
    keep_norm = pltpu.make_async_copy(norm, all_norm.at[me, col], local_sem.at[0])
    keep_norm.start()

    loads = [
        pltpu.make_async_copy(src, dst, local_sem.at[1 + i])
        for i, (src, dst) in enumerate(((gate, own_gate), (up, own_up), (low, own_low), (high, vhigh)))
    ]
    for load in loads:
        load.start()
    for load in loads:
        load.wait()
    stores = [
        pltpu.make_async_copy(src, dst.at[me], local_sem.at[5 + i])
        for i, (src, dst) in enumerate(((own_gate, all_gate), (own_up, all_up), (own_low, all_low)))
    ]
    for store in stores:
        store.start()

    full, rest = divmod(width, LANES)

    def each_block(body):
        def step(t, carry):
            body(t, pl.multiple_of(t * LANES, LANES))
            return carry

        lax.fori_loop(0, full, step, 0)
        if rest:
            body(full, width - LANES)

    for i, shard in enumerate((own_gate, own_up)):
        lower = one_half(own_low, i)

        def add(t, start, shard=shard, lower=lower, i=i):
            at = pl.ds(start, LANES)
            size = jnp.abs(shard[at].astype(jnp.float32) + mix_rate * jnp.dot(
                vhigh[at], lower, preferred_element_type=jnp.float32
            ))
            lanes = sum(size[:, k:k + LANES] for k in range(0, shard.shape[1], LANES))
            part[0, i, pl.ds(t, 1)] = jnp.sum(lanes.T, axis=0, keepdims=True)

        each_block(add)
    keep_norm.wait()

    def exchange(stage, peer):
        held = 1 << stage
        at = pl.ds((me // held) * held, held)
        target = {zero_axis: peer, cols_axis: col}
        go(pltpu.make_async_remote_copy(
            src_ref=part.at[stage], dst_ref=landed.at[stage], send_sem=sum_send.at[stage],
            recv_sem=sum_recv.at[stage], device_id=target, device_id_type=MESH,
        ))
        go(pltpu.make_async_remote_copy(
            src_ref=all_norm.at[at], dst_ref=all_norm.at[at], send_sem=norm_send.at[stage],
            recv_sem=norm_recv.at[stage], device_id=target, device_id_type=MESH,
        ))

    def finish(stage, peer):
        held = 1 << stage
        at = pl.ds((peer // held) * held, held)
        pltpu.make_async_copy(landed.at[stage], landed.at[stage], sum_recv.at[stage]).wait()
        pltpu.make_async_copy(all_norm.at[at], all_norm.at[at], norm_recv.at[stage]).wait()
        summed = part[stage] + landed[stage]
        if stage < 2:
            part[stage + 1] = summed
            return
        total[...] = summed
        for i in range(2):
            def spread(t, start, i=i):
                row = jnp.broadcast_to(total[i, pl.ds(t, 1)], (LANES, LANES))
                scale[i, pl.ds(start, LANES)] = 1.0 / (row.T / d_model)

            each_block(spread)

    def arrived(kind, p, owner):
        here = place(p, owner)
        pltpu.make_async_copy(here, here, recv.at[kind, p]).wait()

    def diag_arrived(p):
        arrived(DIAG, p, diag)
        go(copy(D_S, p, place(p, diag), diag, sib))

    for p in range(count):
        arrived(OWN_X, p, xn)
        if p + WINDOW < count:
            send_own(p + WINDOW)
        if p % 2 == 0:
            go(copy(DIAG, p, place(p, xn), xn, yn))
        go(copy(X_S, p, place(p, xn), xn, sib))
        arrived(OWN_Y, p, yn)
        if p % 2 == 1:
            go(copy(DIAG, p, place(p, yn), yn, xn))
        go(copy(Y_S, p, place(p, yn), yn, sib))
        if p == 1:
            for step in range(1, cols):
                back = all_norm.at[me, (col + cols - step) % cols]
                pltpu.make_async_copy(back, back, z_recv.at[step]).wait()
            exchange(0, sib)
        if p == 3:
            finish(0, sib)
        if p == 4:
            exchange(1, xn)
        if p == count - 3:
            finish(1, xn)
        if p == count - 2:
            exchange(2, yn)
    for p in range(count - 1):
        diag_arrived(p)
    finish(2, yn)
    diag_arrived(count - 1)
    for p in range(count):
        arrived(OWN_S, p, sib)
        arrived(X_S, p, sib + to_x)
        arrived(Y_S, p, sib + to_y)
        arrived(D_S, p, sib + to_x + to_y)
    for store in stores:
        store.wait()
    for c in started:
        c.wait_send()


def merge_kernel(gate, up, low, high, scale, out_gate, out_up):
    lanes = gate.shape[1]
    for i, (shard, out) in enumerate(((gate, out_gate), (up, out_up))):
        lower = one_half(low, i)

        latest = shard[...].astype(jnp.float32) + mix_rate * jnp.dot(
            high[...], lower, preferred_element_type=jnp.float32
        )
        by = scale[i]
        for k in range(0, lanes, LANES):
            out[:, k:k + LANES] = (latest[:, k:k + LANES] * by).astype(out.dtype)


def merge(all_gate, all_up, all_low, high, scale):
    n, width, lanes = all_gate.shape
    block = next(width // c for c in range(1, width) if width % (c * TILE) == 0 and width // c <= BLOCK)
    shard = pl.BlockSpec((None, block, lanes), lambda r, b: (b, r, 0))
    out = pl.BlockSpec((block, lanes), lambda r, b: (r, b))
    return pl.pallas_call(
        merge_kernel,
        grid=(width // block, n),
        in_specs=[
            shard,
            shard,
            pl.BlockSpec((None,) + all_low.shape[1:], lambda r, b: (b, 0, 0)),
            pl.BlockSpec((block, high.shape[1]), lambda r, b: (r, 0)),
            pl.BlockSpec((2, block, LANES), lambda r, b: (0, r, 0)),
        ],
        out_specs=[out, out],
        out_shape=[jax.ShapeDtypeStruct((width, n * lanes), jnp.bfloat16)] * 2,
        compiler_params=pltpu.CompilerParams(vmem_limit_bytes=40 * 1024 * 1024),
    )(all_gate, all_up, all_low, high, scale)


def gathered(mesh, gate, up, low, high, stepped):
    n, cols = mesh.shape["zero"], mesh.shape["cols"]
    width, lanes = gate.shape
    piece = jnp.broadcast_to(stepped[None, :], (8, stepped.shape[0]))
    count = 2 * CHUNKS + 2
    lines = pl.cdiv(width, LANES)
    anywhere = pl.BlockSpec(memory_space=pl.ANY)
    vmem = pl.BlockSpec(memory_space=pltpu.VMEM)
    dma = lambda *shape: pltpu.SemaphoreType.DMA(shape)
    return pl.pallas_call(
        functools.partial(gather_kernel, n, cols, ("zero", "cols")),
        in_specs=[anywhere] * 4 + [vmem],
        out_specs=[anywhere] * 3 + [vmem] * 3,
        out_shape=[
            jax.ShapeDtypeStruct((n,) + gate.shape, jnp.bfloat16),
            jax.ShapeDtypeStruct((n,) + gate.shape, jnp.bfloat16),
            jax.ShapeDtypeStruct((n,) + low.shape, jnp.bfloat16),
            jax.ShapeDtypeStruct((2, lines, LANES), jnp.float32),
            jax.ShapeDtypeStruct((2, width, LANES), jnp.float32),
            jax.ShapeDtypeStruct((n, cols) + piece.shape, jnp.float32),
        ],
        scratch_shapes=[
            pltpu.VMEM(gate.shape, jnp.bfloat16),
            pltpu.VMEM(gate.shape, jnp.bfloat16),
            pltpu.VMEM(low.shape, jnp.bfloat16),
            pltpu.VMEM(high.shape, jnp.bfloat16),
            pltpu.VMEM((3, 2, lines, LANES), jnp.float32),
            pltpu.VMEM((3, 2, lines, LANES), jnp.float32),
            dma(7, count), dma(7, count), dma(8),
            dma(3), dma(3), dma(3), dma(3), dma(cols), dma(cols),
        ],
        compiler_params=pltpu.CompilerParams(collective_id=0, has_side_effects=True),
    )(gate, up, low, high, piece)


def shards(mesh, train_gate, low_gate, high_gate, train_up, low_up, high_up, norm_train, norm_step):
    low = jnp.concatenate([low_gate.T, low_up.T], axis=0)
    high = jnp.concatenate([high_gate, high_up], axis=0).T
    all_gate, all_up, all_low, total, scale, all_norm = gathered(
        mesh, train_gate.T, train_up.T, low, high, norm_train + norm_step
    )
    ready_gate, ready_up = merge(all_gate, all_up, all_low, high, scale)
    width = high.shape[0]
    full, rest = divmod(width, LANES)
    sums = total[:, :full].reshape(2, -1)
    if rest:
        sums = jnp.concatenate([sums, total[:, full, LANES - rest:]], axis=1)
    factors = sums / ready_gate.shape[1]
    serve_norm = all_norm[:, :, 0, :].reshape(-1).astype(jnp.bfloat16)
    return ready_gate.T, ready_up.T, factors[0], factors[1], serve_norm


def shards_any(mesh, train_gate, low_gate, high_gate, train_up, low_up, high_up, norm_train, norm_step):
    def sums(train, low, high):
        latest = train.astype(jnp.float32) + mix_rate * jnp.dot(low, high, preferred_element_type=jnp.float32)
        return jnp.sum(jnp.abs(latest), axis=0)

    gather = lambda a: lax.all_gather(a, "zero", axis=0)
    low = jnp.concatenate([low_gate.T, low_up.T], axis=0)
    high = jnp.concatenate([high_gate, high_up], axis=0).T
    all_gate, all_up, all_low = gather(train_gate.T), gather(train_up.T), gather(low)
    total = lax.psum(jnp.stack([sums(train_gate, low_gate, high_gate), sums(train_up, low_up, high_up)]), "zero")
    factors = total / (mesh.shape["zero"] * train_gate.shape[0])
    scale = jnp.broadcast_to((1.0 / factors)[:, :, None], factors.shape + (LANES,))
    ready_gate, ready_up = merge(all_gate, all_up, all_low, high, scale)
    serve_norm = lax.all_gather(
        (norm_train + norm_step).astype(jnp.bfloat16), ("zero", "cols"), axis=0, tiled=True
    )
    return ready_gate.T, ready_up.T, factors[0], factors[1], serve_norm


def solution(mesh):
    body = shards if mesh.shape["zero"] == 1 << 3 else shards_any
    return jax.shard_map(
        functools.partial(body, mesh),
        mesh=mesh,
        in_specs=(
            P("zero", "cols"),
            P("zero", None),
            P(None, "cols"),
            P("zero", "cols"),
            P("zero", None),
            P(None, "cols"),
            P(("zero", "cols")),
            P(("zero", "cols")),
        ),
        out_specs=(P(None, "cols"), P(None, "cols"), P("cols"), P("cols"), P()),
        check_vma=False,
    )
```
